32 devices in a mesh: cfg: 2 (over y), space: 4 (over z), tm: 4 (over x, core).
Axes of the slice: x: 2, y: 2, z: 4, core: 2. Of those that a mesh axis runs over, the one named last changes fastest.
Arguments:
- solutions: bfloat16 [16, 128, 32, 3072], P(('cfg', 'tm'), None, None, 'space'), parts along dimension 0, may hold values from -6 to 6
- eigvecs: bfloat16 [16, 2, 128, 3072], P(('cfg', 'tm'), None, 'space'), parts along dimension 0, may hold values from -0.078125 to 0.078125
- source_time: int32 [256], P('cfg'), parts along dimension 0, may hold values from 0 to 7
Outputs:
- perambulator: bfloat16 [16, 128, 32, 128], P(('cfg', 'tm'), 'space'), parts along dimension 0
The draws below stay inside these ranges and needn't reach their ends.
There are 2 independent parts, one for each index of `cfg`. The reference program is written for one: setup_inputs(seed, part) draws one part's arguments, and reference() takes and returns one part's arrays. A program takes and returns all parts, laid end to end along the dimension named above; each array names one. Nothing has to cross between parts.
All inputs are finite; a program needn't handle non-finite values.
Results may differ from the reference program's by a relative error of at most 0.001.
Values may be sent and summed in bfloat16 or wider, within the bound.
A program may use at most 128 MiB of HBM per device.

```python
import jax
import jax.numpy as jnp
from jax import lax

NVEC = 128
NSRC = 128
NT = 8
CV = 3072


def place_ends(array, key, low, high):
    extent = array.shape
    spot = [jax.random.randint(jax.random.fold_in(key, axis), (), 0, extent[axis]) for axis in range(len(extent))]
    array = array.at[tuple(spot)].set(low)
    longest = extent.index(max(extent))
    spot[longest] = (spot[longest] + 1) % extent[longest]
    return array.at[tuple(spot)].set(high)


def strengthened(values, key, source, target, blocks, factor):
    owner, partner = [(jnp.arange(values.shape[position]) // (values.shape[position] // blocks)).reshape([-1 if axis == position else 1 for axis in range(values.ndim)]) for position in (source, target)]
    chosen = jax.random.permutation(key, blocks)[partner]
    strong = (owner == chosen) | (owner == (partner + blocks // 2) % blocks)
    return jnp.where(strong, factor * values, values)


def shard_levels(key, dims, cuts, low, high):
    def one(dim, parts):
        steps = jax.random.uniform(jax.random.fold_in(jax.random.fold_in(key, 6), dim), (parts,), jnp.float32, low / len(cuts), high / len(cuts))
        return jnp.repeat(jnp.exp(steps), dims[dim] // parts).reshape((-1,) + (1,) * (len(dims) - dim - 1))

    factor_of = one(*cuts[0])
    for cut in cuts[1:]:
        factor_of = factor_of * one(*cut)
    return factor_of


def gaussian(own_key, extent, width, limit, cuts=(), kind=jnp.bfloat16):
    drawn = width * jax.random.normal(own_key, extent, jnp.float32)
    if cuts:
        drawn = drawn * shard_levels(own_key, extent, cuts, -0.22, 0.18)
    return jnp.clip(drawn, -limit, limit).astype(kind)


def heavy_noise(rng, dims, spread, bound, cuts, heavy, kind=jnp.bfloat16):
    drawn = spread * jax.random.normal(rng, dims, jnp.float32)
    if cuts:
        drawn = drawn * shard_levels(rng, dims, cuts, -0.22, 0.18)
    return jnp.clip(strengthened(drawn, jax.random.fold_in(rng, 3), *heavy), -bound, bound).astype(kind)


def setup_inputs(seed: int = 0, part: int = 0) -> dict:
    key_of = jax.random.split(jax.random.key(seed), 4)
    part_splits = jax.random.split(jax.random.fold_in(key_of[3], part), 4)
    solutions = heavy_noise(part_splits[0], (NT, NSRC, 32, CV), 1.0, 6.0, ((0, 4), (3, 4)), (3, 1, 4, 2.0))
    eigvecs = gaussian(part_splits[1], (NT, 2, NVEC, CV), (2 * CV) ** -0.5, 0.078125, ((0, 4), (2, 4)))
    source_time = place_ends(jax.random.randint(part_splits[2], (NSRC,), 0, NT), jax.random.fold_in(part_splits[2], 1), 0, NT - 1).astype(jnp.int32)
    return {"solutions": solutions, "eigvecs": eigvecs, "source_time": source_time}


def contract_slice(spinors, vectors):
    sources = spinors.shape[0]
    count = vectors.shape[1]
    stacked = vectors.reshape(2 * count, vectors.shape[2])
    products = jnp.dot(spinors.reshape(sources * 32, spinors.shape[2]), stacked.T, precision=lax.Precision.HIGHEST, preferred_element_type=jnp.float32)
    products = products.reshape(sources, 2, 16, 2, count)
    real_part = products[:, 0, :, 0, :] + products[:, 1, :, 1, :]
    imag_part = products[:, 1, :, 0, :] - products[:, 0, :, 1, :]
    return jnp.concatenate([real_part, imag_part], axis=1)


def reference(solutions, eigvecs, source_time):
    def one_slice(pair):
        return contract_slice(pair[0].astype(jnp.float32), pair[1].astype(jnp.float32))

    sums = lax.map(one_slice, (solutions, eigvecs))
    times = jnp.arange(NT, dtype=jnp.int32)
    signs = jnp.where(times[:, None] < source_time[None, :], -1.0, 1.0).astype(jnp.float32)
    return (sums * signs[:, :, None, None]).astype(jnp.bfloat16)
```

```python
import functools

import jax
import jax.numpy as jnp
from jax import lax
from jax.experimental import pallas as pl
from jax.experimental.pallas import tpu as pltpu
from jax.sharding import PartitionSpec as P

MESH = pl.DeviceIdType.MESH
LEVELS = 32767.0
PIECES = 1
VMEM_BYTES = 67043328


def kernel(n, pieces, time_hbm, sol_hbm, eig_hbm, out_ref, time_ref, eig_v, sol_v, part, own, code, code_in, head,
           head_in, time_sem, load_sem, sol_sem, eig_send, eig_recv, code_send, code_recv, head_send, head_recv):
    me = lax.axis_index("space")
    slices, sources, spins, cols = sol_v.shape
    count = eig_v.shape[4]
    vectors = n * count
    owned = sources // n
    piece = owned // pieces
    rows = piece * spins
    half = spins // 2
    blocks = slices * pieces
    mirror = n - 1 - me

    barrier = pltpu.get_barrier_semaphore()

    def next_of(way):
        return me + 1 if way == 0 else me - 1

    def behind(way):
        return me if way == 0 else mirror

    for way in range(2):
        @pl.when(behind(1 - way) > 0)
        def _():
            pl.semaphore_signal(barrier, inc=1, device_id={"space": next_of(way)}, device_id_type=MESH)

    def eig_load(t, d):
        block = pl.ds(pl.multiple_of(d * cols, cols), cols)
        return pltpu.make_async_copy(eig_hbm.at[t, :, :, block], eig_v.at[t, d, :, me], load_sem.at[t, d])

    def sol_copy(t, d):
        owner = pl.ds(d * owned, owned)
        return pltpu.make_async_copy(sol_hbm.at[t, owner], sol_v.at[t, owner], sol_sem.at[t, d])

    def eig_copy(way, t, d, c, s):
        return pltpu.make_async_remote_copy(
            eig_v.at[t, d, c, s], eig_v.at[t, d, c, s], eig_send.at[t, d, c, s], eig_recv.at[t, d, c, s],
            device_id={"space": next_of(way)}, device_id_type=MESH)

    def each(total, body):
        def step(i, _):
            body(i)
            return 0
        lax.fori_loop(0, total, step, 0)

    each(slices * n, lambda i: eig_load(i % slices, i // slices).start())
    time_copy = pltpu.make_async_copy(time_hbm, time_ref, time_sem)
    time_copy.start()
    each(slices * n, lambda i: eig_load(i % slices, i // slices).wait())
    pl.semaphore_wait(barrier, jnp.where((me > 0) & (mirror > 0), 2, 1))

    def message(way, i):
        members = behind(way) + 1
        slot = i // members
        t, far, back = slot % slices, slot // slices, i % members
        if way == 0:
            return t, n - 1 - far, me - back, far < mirror
        return t, far, me + back, far < me

    def send_eigs(i):
        for c in range(2):
            for way in range(2):
                t, d, s, valid = message(way, i)

                @pl.when(valid)
                def _():
                    @pl.when(s != me)
                    def _():
                        eig_copy(way, t, d, c, s).wait_recv()

                    eig_copy(way, t, d, c, s).start()

    send_eigs(0)
    each(slices * n, lambda i: sol_copy(i // n, i % n).start())
    messages = slices * ((n * n) // 4)
    each(messages - 1, lambda i: send_eigs(i + 1))

    def wait_eigs(t):
        def body(i):
            s = i // 2

            @pl.when(s != me)
            def _():
                eig_copy(0, t, me, i % 2, s).wait_recv()

        each(2 * n, body)

    wait_eigs(0)
    each(slices * n, lambda i: sol_copy(i // n, i % n).wait())
    time_copy.wait()

    def partial_sum(t, q, dst):
        block = sol_v[t, pl.ds(q * piece, piece)].reshape(rows, cols)
        w = eig_v[t, me]
        if count % 16:
            w = w.astype(jnp.float32)
        w = w.reshape(2 * vectors, cols).astype(jnp.bfloat16)
        p = lax.dot_general(block, w, (((1,), (1,)), ((), ())), preferred_element_type=jnp.float32)
        p = p.reshape(piece, 2, half, 2 * vectors)
        dst[:, :half, :] = p[:, 0, :, :vectors] + p[:, 1, :, vectors:]
        dst[:, half:, :] = p[:, 1, :, :vectors] - p[:, 0, :, vectors:]

    def chunk_copy(way, t, q):
        return pltpu.make_async_remote_copy(
            code.at[t, q], code_in.at[way, t, q], code_send.at[t, q], code_recv.at[way, t, q],
            device_id={"space": jnp.where(way == 0, me + 1, me - 1)}, device_id_type=MESH)

    def head_copy(way, t, q):
        return pltpu.make_async_remote_copy(
            head.at[t, q], head_in.at[way, t, q], head_send.at[t, q], head_recv.at[way, t, q],
            device_id={"space": jnp.where(way == 0, me + 1, me - 1)}, device_id_type=MESH)

    def received(way, t, q):
        head_copy(way, t, q).wait_recv()
        chunk_copy(way, t, q).wait_recv()
        value = code_in[way, t, q].astype(jnp.int32).astype(jnp.float32) * head_in[way, t, q]
        return value.reshape(piece, spins, vectors)

    def emit(way, i):
        far, t, k = i // blocks, (i // pieces) % slices, i % pieces
        d = jnp.where(way == 0, n - 1 - far, far)
        q = d * pieces + k
        partial_sum(t, q, part)

        @pl.when(jnp.where(way == 0, me, mirror) > 0)
        def _():
            part[...] += received(way, t, q)

        x = part[...].reshape(rows, vectors)
        top = jnp.maximum(jnp.max(jnp.abs(x), axis=0, keepdims=True), 1e-30)
        head[t, q] = top * (1.0 / LEVELS)
        code[t, q] = jnp.round(x * (LEVELS / top)).astype(jnp.int32).astype(jnp.int16)
        head_copy(way, t, q).start()
        chunk_copy(way, t, q).start()

    lower = me < n // 2
    early = jnp.where(lower, 0, 1)
    late = 1 - early
    lead = blocks * jnp.where(lower, mirror - me, me - mirror)
    many = blocks * jnp.where(lower, mirror, me)
    few = blocks * jnp.where(lower, me, mirror)

    def emit_step(j):
        if slices > 1:
            @pl.when(j == pieces)
            def _():
                for t in range(1, slices):
                    wait_eigs(t)

        @pl.when((j >= lead) & (j - lead < few))
        def _():
            emit(late, j - lead)

        @pl.when(j < many)
        def _():
            emit(early, j)

    each(blocks * (n - 1), emit_step)

    each(blocks, lambda j: partial_sum(j // pieces, me * pieces + j % pieces, own.at[j // pieces, j % pieces]))

    @pl.when(jnp.where(lower, mirror, me) > 0)
    def _():
        def body(j):
            t, i = j // pieces, j % pieces
            own[t, i] += received(late, t, me * pieces + i)
        each(blocks, body)

    def finish(j):
        t, i = j // pieces, j % pieces

        @pl.when(jnp.where(lower, me, mirror) > 0)
        def _():
            own[t, i] += received(early, t, me * pieces + i)

        now = lax.axis_index("tm") * slices + t
        for b in range(piece):
            sign = jnp.where(now < time_ref[me * owned + i * piece + b], -1.0, 1.0)
            out_ref[t, i * piece + b] = (own[t, i, b] * sign).astype(jnp.bfloat16)

    each(blocks, finish)

    def drain_eigs(i):
        for c in range(2):
            for way in range(2):
                t, d, s, valid = message(way, i)

                @pl.when(valid)
                def _():
                    eig_copy(way, t, d, c, s).wait_send()

    each(messages, drain_eigs)

    def drain(j):
        t, q = j // (n * pieces), j % (n * pieces)
        d = q // pieces

        @pl.when(d != me)
        def _():
            way = jnp.where(d > me, 0, 1)
            head_copy(way, t, q).wait_send()
            chunk_copy(way, t, q).wait_send()

    each(slices * n * pieces, drain)


def shards(n, solutions, eigvecs, source_time):
    slices, sources, spins, cols = solutions.shape
    count = eigvecs.shape[2]
    vectors = n * count
    owned = sources // n
    pieces = PIECES if owned % PIECES == 0 else 1
    piece = owned // pieces
    blocks = n * pieces
    dma = pltpu.SemaphoreType.DMA
    result = jax.ShapeDtypeStruct((slices, owned, spins, vectors), jnp.bfloat16)
    return pl.pallas_call(
        functools.partial(kernel, n, pieces),
        out_shape=result,
        in_specs=[
            pl.BlockSpec(memory_space=pltpu.HBM),
            pl.BlockSpec(memory_space=pltpu.HBM),
            pl.BlockSpec(memory_space=pltpu.HBM),
        ],
        out_specs=pl.BlockSpec(memory_space=pltpu.VMEM),
        scratch_shapes=[
            pltpu.SMEM(source_time.shape, jnp.int32),
            pltpu.VMEM((slices, n, 2, n, count, cols), jnp.bfloat16),
            pltpu.VMEM((slices, sources, spins, cols), jnp.bfloat16),
            pltpu.VMEM((piece, spins, vectors), jnp.float32),
            pltpu.VMEM((slices, pieces, piece, spins, vectors), jnp.float32),
            pltpu.VMEM((slices, blocks, piece * spins, vectors), jnp.int16),
            pltpu.VMEM((2, slices, blocks, piece * spins, vectors), jnp.int16),
            pltpu.VMEM((slices, blocks, 1, vectors), jnp.float32),
            pltpu.VMEM((2, slices, blocks, 1, vectors), jnp.float32),
            dma,
            dma((slices, n)),
            dma((slices, n)),
            dma((slices, n, 2, n)),
            dma((slices, n, 2, n)),
            dma((slices, blocks)),
            dma((2, slices, blocks)),
            dma((slices, blocks)),
            dma((2, slices, blocks)),
        ],
        compiler_params=pltpu.CompilerParams(
            collective_id=0, has_side_effects=True, vmem_limit_bytes=VMEM_BYTES - result.size * 2),
    )(source_time, solutions, eigvecs)


def solution(mesh):
    return jax.shard_map(
        functools.partial(shards, mesh.shape["space"]),
        mesh=mesh,
        in_specs=(
            P(("cfg", "tm"), None, None, "space"),
            P(("cfg", "tm"), None, "space", None),
            P("cfg"),
        ),
        out_specs=P(("cfg", "tm"), "space", None, None),
        check_vma=False,
    )
```

```python
import functools

import jax
import jax.numpy as jnp
from jax import lax
from jax.experimental import pallas as pl
from jax.experimental.pallas import tpu as pltpu
from jax.sharding import PartitionSpec as P

MESH = pl.DeviceIdType.MESH
LEVELS = 32767.0
PIECES = 1
VMEM_BYTES = 48 << 20


def kernel(n, pieces, time_hbm, sol_hbm, eig_hbm, out_ref, time_ref, eig_v, sol_v, sign, part, own, code, code_in,
           head, head_in, time_sem, load_sem, sol_sem, eig_send, eig_recv, code_send, code_recv, head_send, head_recv):
    me = lax.axis_index("space")
    slices, sources, spins, cols = sol_v.shape
    count = eig_v.shape[4]
    vectors = n * count
    owned = sources // n
    piece = owned // pieces
    rows = piece * spins
    half = spins // 2
    blocks = slices * pieces
    mirror = n - 1 - me

    barrier = pltpu.get_barrier_semaphore()

    def next_of(way):
        return me + 1 if way == 0 else me - 1

    def behind(way):
        return me if way == 0 else mirror

    for way in range(2):
        @pl.when(behind(1 - way) > 0)
        def _():
            pl.semaphore_signal(barrier, inc=1, device_id={"space": next_of(way)}, device_id_type=MESH)

    def eig_load(t, d):
        block = pl.ds(pl.multiple_of(d * cols, cols), cols)
        return pltpu.make_async_copy(eig_hbm.at[t, :, :, block], eig_v.at[t, d, :, me], load_sem.at[t, d])

    def sol_copy(t, d):
        owner = pl.ds(d * owned, owned)
        return pltpu.make_async_copy(sol_hbm.at[t, owner], sol_v.at[t, owner], sol_sem.at[t, d])

    def eig_copy(way, t, d, c, s):
        return pltpu.make_async_remote_copy(
            eig_v.at[t, d, c, s], eig_v.at[t, d, c, s], eig_send.at[t, d, c, s], eig_recv.at[t, d, c, s],
            device_id={"space": next_of(way)}, device_id_type=MESH)

    def each(total, body):
        def step(i, _):
            body(i)
            return 0
        lax.fori_loop(0, total, step, 0)

    def load_eigs(i):
        far, t = i // slices, i % slices
        for d in (n - 1 - far, far):
            eig_load(t, d).start()

    each(slices * (n // 2), load_eigs)
    if n % 2:
        each(slices, lambda t: eig_load(t, n // 2).start())
    time_copy = pltpu.make_async_copy(time_hbm, time_ref, time_sem)
    time_copy.start()
    pl.semaphore_wait(barrier, jnp.where((me > 0) & (mirror > 0), 2, 1))

    def message(way, i):
        members = behind(way) + 1
        slot = i // members
        t, far, back = slot % slices, slot // slices, i % members
        if way == 0:
            return t, n - 1 - far, me - back, far < mirror
        return t, far, me + back, far < me

    def send_eigs(i):
        for c in range(2):
            for way in range(2):
                t, d, s, valid = message(way, i)

                @pl.when(valid)
                def _():
                    @pl.when(s != me)
                    def _():
                        eig_copy(way, t, d, c, s).wait_recv()

                    if c == 0:
                        @pl.when(s == me)
                        def _():
                            eig_load(t, d).wait()

                    eig_copy(way, t, d, c, s).start()

    send_eigs(0)
    each(slices * n, lambda i: sol_copy(i // n, i % n).start())
    messages = slices * ((n * n) // 4)
    each(messages - 1, lambda i: send_eigs(i + 1))

    def wait_eigs(t):
        eig_load(t, me).wait()

        def body(i):
            s = i // 2

            @pl.when(s != me)
            def _():
                eig_copy(0, t, me, i % 2, s).wait_recv()

        each(2 * n, body)

    wait_eigs(0)
    each(slices * n, lambda i: sol_copy(i // n, i % n).wait())

    def partial_sum(t, q, dst):
        block = sol_v[t, pl.ds(q * piece, piece)].reshape(rows, cols)
        w = eig_v[t, me]
        if count % 16:
            w = w.astype(jnp.float32)
        w = w.reshape(2 * vectors, cols).astype(jnp.bfloat16)
        p = lax.dot_general(block, w, (((1,), (1,)), ((), ())), preferred_element_type=jnp.float32)
        p = p.reshape(piece, 2, half, 2 * vectors)
        dst[:, :half, :] = p[:, 0, :, :vectors] + p[:, 1, :, vectors:]
        dst[:, half:, :] = p[:, 1, :, :vectors] - p[:, 0, :, vectors:]

    def chunk_copy(way, t, q):
        return pltpu.make_async_remote_copy(
            code.at[t, q], code_in.at[way, t, q], code_send.at[t, q], code_recv.at[way, t, q],
            device_id={"space": jnp.where(way == 0, me + 1, me - 1)}, device_id_type=MESH)

    def head_copy(way, t, q):
        return pltpu.make_async_remote_copy(
            head.at[t, q], head_in.at[way, t, q], head_send.at[t, q], head_recv.at[way, t, q],
            device_id={"space": jnp.where(way == 0, me + 1, me - 1)}, device_id_type=MESH)

    def received(way, t, q):
        head_copy(way, t, q).wait_recv()
        chunk_copy(way, t, q).wait_recv()
        value = code_in[way, t, q].astype(jnp.int32).astype(jnp.float32) * head_in[way, t, q]
        return value.reshape(piece, spins, vectors)

    def emit(way, i):
        far, t, k = i // blocks, (i // pieces) % slices, i % pieces
        d = jnp.where(way == 0, n - 1 - far, far)
        q = d * pieces + k
        partial_sum(t, q, part)

        @pl.when(jnp.where(way == 0, me, mirror) > 0)
        def _():
            part[...] += received(way, t, q)

        x = part[...].reshape(rows, vectors)
        top = jnp.maximum(jnp.max(jnp.abs(x), axis=0, keepdims=True), 1e-30)
        head[t, q] = top * (1.0 / LEVELS)
        code[t, q] = jnp.round(x * (LEVELS / top)).astype(jnp.int32).astype(jnp.int16)
        head_copy(way, t, q).start()
        chunk_copy(way, t, q).start()

    lower = me < n // 2
    early = jnp.where(lower, 0, 1)
    late = 1 - early
    lead = blocks * jnp.where(lower, mirror - me, me - mirror)
    many = blocks * jnp.where(lower, mirror, me)
    few = blocks * jnp.where(lower, me, mirror)

    def emit_step(j):
        if slices > 1:
            @pl.when(j == pieces)
            def _():
                for t in range(1, slices):
                    wait_eigs(t)

        @pl.when((j >= lead) & (j - lead < few))
        def _():
            emit(late, j - lead)

        @pl.when(j < many)
        def _():
            emit(early, j)

    each(blocks * (n - 1), emit_step)

    time_copy.wait()

    def set_sign(j):
        t, b = j // owned, j % owned
        now = lax.axis_index("tm") * slices + t
        value = jnp.where(now < time_ref[me * owned + b], -1.0, 1.0)
        sign[t, b] = jnp.full((1, vectors), value, jnp.float32)

    each(slices * owned, set_sign)
    each(blocks, lambda j: partial_sum(j // pieces, me * pieces + j % pieces, own.at[j // pieces, j % pieces]))

    @pl.when(jnp.where(lower, mirror, me) > 0)
    def _():
        def body(j):
            t, i = j // pieces, j % pieces
            own[t, i] += received(late, t, me * pieces + i)
        each(blocks, body)

    def drain_eigs(i):
        for c in range(2):
            for way in range(2):
                t, d, s, valid = message(way, i)

                @pl.when(valid)
                def _():
                    eig_copy(way, t, d, c, s).wait_send()

    each(messages, drain_eigs)

    def drain(j):
        t, q = j // (n * pieces), j % (n * pieces)
        d = q // pieces

        @pl.when(d != me)
        def _():
            way = jnp.where(d > me, 0, 1)
            head_copy(way, t, q).wait_send()
            chunk_copy(way, t, q).wait_send()

    each(slices * n * pieces, drain)

    def finish(j):
        t, i = j // pieces, j % pieces

        @pl.when(jnp.where(lower, me, mirror) > 0)
        def _():
            own[t, i] += received(early, t, me * pieces + i)

        mine = pl.ds(i * piece, piece)
        out_ref[t, mine] = (own[t, i] * sign[t, mine]).astype(jnp.bfloat16)

    each(blocks, finish)


def shards(n, solutions, eigvecs, source_time):
    slices, sources, spins, cols = solutions.shape
    count = eigvecs.shape[2]
    vectors = n * count
    owned = sources // n
    pieces = PIECES if owned % PIECES == 0 else 1
    piece = owned // pieces
    blocks = n * pieces
    dma = pltpu.SemaphoreType.DMA
    result = jax.ShapeDtypeStruct((slices, owned, spins, vectors), jnp.bfloat16)
    return pl.pallas_call(
        functools.partial(kernel, n, pieces),
        out_shape=result,
        in_specs=[
            pl.BlockSpec(memory_space=pltpu.HBM),
            pl.BlockSpec(memory_space=pltpu.HBM),
            pl.BlockSpec(memory_space=pltpu.HBM),
        ],
        out_specs=pl.BlockSpec(memory_space=pltpu.VMEM),
        scratch_shapes=[
            pltpu.SMEM(source_time.shape, jnp.int32),
            pltpu.VMEM((slices, n, 2, n, count, cols), jnp.bfloat16),
            pltpu.VMEM((slices, sources, spins, cols), jnp.bfloat16),
            pltpu.VMEM((slices, owned, 1, vectors), jnp.float32),
            pltpu.VMEM((piece, spins, vectors), jnp.float32),
            pltpu.VMEM((slices, pieces, piece, spins, vectors), jnp.float32),
            pltpu.VMEM((slices, blocks, piece * spins, vectors), jnp.int16),
            pltpu.VMEM((2, slices, blocks, piece * spins, vectors), jnp.int16),
            pltpu.VMEM((slices, blocks, 1, vectors), jnp.float32),
            pltpu.VMEM((2, slices, blocks, 1, vectors), jnp.float32),
            dma,
            dma((slices, n)),
            dma((slices, n)),
            dma((slices, n, 2, n)),
            dma((slices, n, 2, n)),
            dma((slices, blocks)),
            dma((2, slices, blocks)),
            dma((slices, blocks)),
            dma((2, slices, blocks)),
        ],
        compiler_params=pltpu.CompilerParams(
            collective_id=0, has_side_effects=True, vmem_limit_bytes=VMEM_BYTES),
    )(*(pltpu.with_memory_space_constraint(x, pltpu.HBM) for x in (source_time, solutions, eigvecs)))


def solution(mesh):
    return jax.shard_map(
        functools.partial(shards, mesh.shape["space"]),
        mesh=mesh,
        in_specs=(
            P(("cfg", "tm"), None, None, "space"),
            P(("cfg", "tm"), None, "space", None),
            P("cfg"),
        ),
        out_specs=P(("cfg", "tm"), "space", None, None),
        check_vma=False,
    )
```

```python
import functools

import jax
import jax.numpy as jnp
from jax import lax
from jax.experimental import pallas as pl
from jax.experimental.pallas import tpu as pltpu
from jax.sharding import PartitionSpec as P

MESH = pl.DeviceIdType.MESH
LEVELS = 32767.0
PIECES = 1
VMEM_BYTES = 48 << 20


def kernel(n, pieces, time_hbm, sol_hbm, eig_hbm, out_ref, time_ref, eig_v, sol_v, sign, part, own, code, code_in,
           head, head_in, time_sem, load_sem, sol_sem, eig_send, eig_recv, code_send, code_recv, head_send, head_recv):
    me = lax.axis_index("space")
    slices, sources, spins, cols = sol_v.shape
    count = eig_v.shape[4]
    vectors = n * count
    owned = sources // n
    piece = owned // pieces
    rows = piece * spins
    half = spins // 2
    blocks = slices * pieces
    mirror = n - 1 - me

    barrier = pltpu.get_barrier_semaphore()

    def next_of(way):
        return me + 1 if way == 0 else me - 1

    def behind(way):
        return me if way == 0 else mirror

    for way in range(2):
        @pl.when(behind(1 - way) > 0)
        def _():
            pl.semaphore_signal(barrier, inc=1, device_id={"space": next_of(way)}, device_id_type=MESH)

    def eig_load(t, d):
        block = pl.ds(pl.multiple_of(d * cols, cols), cols)
        return pltpu.make_async_copy(eig_hbm.at[t, :, :, block], eig_v.at[t, d, :, me], load_sem.at[t, d])

    def sol_copy(t, d):
        owner = pl.ds(d * owned, owned)
        return pltpu.make_async_copy(sol_hbm.at[t, owner], sol_v.at[t, owner], sol_sem.at[t, d])

    def eig_copy(way, t, d, c, s):
        return pltpu.make_async_remote_copy(
            eig_v.at[t, d, c, s], eig_v.at[t, d, c, s], eig_send.at[t, d, c, s], eig_recv.at[t, d, c, s],
            device_id={"space": next_of(way)}, device_id_type=MESH)

    def first_copy(way, t, d, c, s):
        block = pl.ds(pl.multiple_of(d * cols, cols), cols)
        return pltpu.make_async_remote_copy(
            eig_hbm.at[t, c, :, block], eig_v.at[t, d, c, s], eig_send.at[t, d, c, s], eig_recv.at[t, d, c, s],
            device_id={"space": next_of(way)}, device_id_type=MESH)

    def each(total, body):
        def step(i, _):
            body(i)
            return 0
        lax.fori_loop(0, total, step, 0)

    def load_eigs(i):
        far, t = i // slices, i % slices
        for d in (n - 1 - far, far):
            @pl.when((t > 0) | (d == me) | ((d != 0) & (d != n - 1)))
            def _():
                eig_load(t, d).start()

    each(slices * (n // 2), load_eigs)
    if n % 2:
        each(slices, lambda t: eig_load(t, n // 2).start())
    time_copy = pltpu.make_async_copy(time_hbm, time_ref, time_sem)
    time_copy.start()
    pl.semaphore_wait(barrier, jnp.where((me > 0) & (mirror > 0), 2, 1))

    def message(way, i):
        members = behind(way) + 1
        slot = i // members
        t, far, back = slot % slices, slot // slices, i % members
        if way == 0:
            return t, n - 1 - far, me - back, far < mirror
        return t, far, me + back, far < me

    def send_eigs(i):
        for c in range(2):
            for way in range(2):
                t, d, s, valid = message(way, i)

                @pl.when(valid)
                def _():
                    @pl.when(s != me)
                    def _():
                        eig_copy(way, t, d, c, s).wait_recv()

                    if c == 0:
                        @pl.when(s == me)
                        def _():
                            eig_load(t, d).wait()

                    eig_copy(way, t, d, c, s).start()

    for c in range(2):
        for way in range(2):
            t, d, s, valid = message(way, 0)

            @pl.when(valid)
            def _():
                first_copy(way, t, d, c, s).start()

    each(slices * n, lambda i: sol_copy(i // n, i % n).start())
    messages = slices * ((n * n) // 4)
    each(messages - 1, lambda i: send_eigs(i + 1))

    def wait_eigs(t):
        eig_load(t, me).wait()

        def body(i):
            s = i // 2

            @pl.when(s != me)
            def _():
                eig_copy(0, t, me, i % 2, s).wait_recv()

        each(2 * n, body)

    wait_eigs(0)
    each(slices * n, lambda i: sol_copy(i // n, i % n).wait())

    def partial_sum(t, q, dst):
        block = sol_v[t, pl.ds(q * piece, piece)].reshape(rows, cols)
        w = eig_v[t, me]
        if count % 16:
            w = w.astype(jnp.float32)
        w = w.reshape(2 * vectors, cols).astype(jnp.bfloat16)
        p = lax.dot_general(block, w, (((1,), (1,)), ((), ())), preferred_element_type=jnp.float32)
        p = p.reshape(piece, 2, half, 2 * vectors)
        dst[:, :half, :] = p[:, 0, :, :vectors] + p[:, 1, :, vectors:]
        dst[:, half:, :] = p[:, 1, :, :vectors] - p[:, 0, :, vectors:]

    def chunk_copy(way, t, q):
        return pltpu.make_async_remote_copy(
            code.at[t, q], code_in.at[way, t, q], code_send.at[t, q], code_recv.at[way, t, q],
            device_id={"space": jnp.where(way == 0, me + 1, me - 1)}, device_id_type=MESH)

    def head_copy(way, t, q):
        return pltpu.make_async_remote_copy(
            head.at[t, q], head_in.at[way, t, q], head_send.at[t, q], head_recv.at[way, t, q],
            device_id={"space": jnp.where(way == 0, me + 1, me - 1)}, device_id_type=MESH)

    def received(way, t, q):
        head_copy(way, t, q).wait_recv()
        chunk_copy(way, t, q).wait_recv()
        value = code_in[way, t, q].astype(jnp.int32).astype(jnp.float32) * head_in[way, t, q]
        return value.reshape(piece, spins, vectors)

    def emit(way, i):
        far, t, k = i // blocks, (i // pieces) % slices, i % pieces
        d = jnp.where(way == 0, n - 1 - far, far)
        q = d * pieces + k
        partial_sum(t, q, part)

        @pl.when(jnp.where(way == 0, me, mirror) > 0)
        def _():
            part[...] += received(way, t, q)

        x = part[...].reshape(rows, vectors)
        top = jnp.maximum(jnp.max(jnp.abs(x), axis=0, keepdims=True), 1e-30)
        head[t, q] = top * (1.0 / LEVELS)
        code[t, q] = jnp.round(x * (LEVELS / top)).astype(jnp.int32).astype(jnp.int16)
        head_copy(way, t, q).start()
        chunk_copy(way, t, q).start()

    lower = me < n // 2
    early = jnp.where(lower, 0, 1)
    late = 1 - early
    lead = blocks * jnp.where(lower, mirror - me, me - mirror)
    many = blocks * jnp.where(lower, mirror, me)
    few = blocks * jnp.where(lower, me, mirror)

    def emit_step(j):
        if slices > 1:
            @pl.when(j == pieces)
            def _():
                for t in range(1, slices):
                    wait_eigs(t)

        @pl.when((j >= lead) & (j - lead < few))
        def _():
            emit(late, j - lead)

        @pl.when(j < many)
        def _():
            emit(early, j)

    each(blocks * (n - 1), emit_step)

    time_copy.wait()

    def set_sign(j):
        t, b = j // owned, j % owned
        now = lax.axis_index("tm") * slices + t
        value = jnp.where(now < time_ref[me * owned + b], -1.0, 1.0)
        sign[t, b] = jnp.full((1, vectors), value, jnp.float32)

    each(slices * owned, set_sign)
    each(blocks, lambda j: partial_sum(j // pieces, me * pieces + j % pieces, own.at[j // pieces, j % pieces]))

    @pl.when(jnp.where(lower, mirror, me) > 0)
    def _():
        def body(j):
            t, i = j // pieces, j % pieces
            own[t, i] += received(late, t, me * pieces + i)
        each(blocks, body)

    def finish(j):
        t, i = j // pieces, j % pieces

        @pl.when(jnp.where(lower, me, mirror) > 0)
        def _():
            own[t, i] += received(early, t, me * pieces + i)

        mine = pl.ds(i * piece, piece)
        out_ref[t, mine] = (own[t, i] * sign[t, mine]).astype(jnp.bfloat16)

    def drain_eigs(i):
        for c in range(2):
            for way in range(2):
                t, d, s, valid = message(way, i)

                @pl.when(valid)
                def _():
                    eig_copy(way, t, d, c, s).wait_send()


    def drain(j):
        t, q = j // (n * pieces), j % (n * pieces)
        d = q // pieces

        @pl.when(d != me)
        def _():
            way = jnp.where(d > me, 0, 1)
            head_copy(way, t, q).wait_send()
            chunk_copy(way, t, q).wait_send()

    outer = (me == 0) | (mirror == 0)

    @pl.when(outer)
    def _():
        each(blocks, finish)

    each(messages, drain_eigs)
    each(slices * n * pieces, drain)

    @pl.when(jnp.logical_not(outer))
    def _():
        each(blocks, finish)


def shards(n, solutions, eigvecs, source_time):
    slices, sources, spins, cols = solutions.shape
    count = eigvecs.shape[2]
    vectors = n * count
    owned = sources // n
    pieces = PIECES if owned % PIECES == 0 else 1
    piece = owned // pieces
    blocks = n * pieces
    dma = pltpu.SemaphoreType.DMA
    result = jax.ShapeDtypeStruct((slices, owned, spins, vectors), jnp.bfloat16)
    return pl.pallas_call(
        functools.partial(kernel, n, pieces),
        out_shape=result,
        in_specs=[
            pl.BlockSpec(memory_space=pltpu.HBM),
            pl.BlockSpec(memory_space=pltpu.HBM),
            pl.BlockSpec(memory_space=pltpu.HBM),
        ],
        out_specs=pl.BlockSpec(memory_space=pltpu.VMEM),
        scratch_shapes=[
            pltpu.SMEM(source_time.shape, jnp.int32),
            pltpu.VMEM((slices, n, 2, n, count, cols), jnp.bfloat16),
            pltpu.VMEM((slices, sources, spins, cols), jnp.bfloat16),
            pltpu.VMEM((slices, owned, 1, vectors), jnp.float32),
            pltpu.VMEM((piece, spins, vectors), jnp.float32),
            pltpu.VMEM((slices, pieces, piece, spins, vectors), jnp.float32),
            pltpu.VMEM((slices, blocks, piece * spins, vectors), jnp.int16),
            pltpu.VMEM((2, slices, blocks, piece * spins, vectors), jnp.int16),
            pltpu.VMEM((slices, blocks, 1, vectors), jnp.float32),
            pltpu.VMEM((2, slices, blocks, 1, vectors), jnp.float32),
            dma,
            dma((slices, n)),
            dma((slices, n)),
            dma((slices, n, 2, n)),
            dma((slices, n, 2, n)),
            dma((slices, blocks)),
            dma((2, slices, blocks)),
            dma((slices, blocks)),
            dma((2, slices, blocks)),
        ],
        compiler_params=pltpu.CompilerParams(
            collective_id=0, has_side_effects=True, vmem_limit_bytes=VMEM_BYTES),
    )(*(pltpu.with_memory_space_constraint(x, pltpu.HBM) for x in (source_time, solutions, eigvecs)))


def solution(mesh):
    return jax.shard_map(
        functools.partial(shards, mesh.shape["space"]),
        mesh=mesh,
        in_specs=(
            P(("cfg", "tm"), None, None, "space"),
            P(("cfg", "tm"), None, "space", None),
            P("cfg"),
        ),
        out_specs=P(("cfg", "tm"), "space", None, None),
        check_vma=False,
    )
```

```python
import functools

import jax
import jax.numpy as jnp
from jax import lax
from jax.experimental import pallas as pl
from jax.experimental.pallas import tpu as pltpu
from jax.sharding import PartitionSpec as P

MESH = pl.DeviceIdType.MESH
LEVELS = 32767.0
PIECES = 1
VMEM_BYTES = 48 << 20


def kernel(n, pieces, time_hbm, sol_hbm, eig_hbm, out_ref, time_ref, eig_v, sol_v, sign, part, own, code, code_in,
           head, head_in, time_sem, load_sem, sol_sem, eig_send, eig_recv, code_send, code_recv, head_send, head_recv):
    me = lax.axis_index("space")
    slices, sources, spins, cols = sol_v.shape
    count = eig_v.shape[4]
    vectors = n * count
    owned = sources // n
    piece = owned // pieces
    rows = piece * spins
    half = spins // 2
    blocks = slices * pieces
    mirror = n - 1 - me

    barrier = pltpu.get_barrier_semaphore()

    def next_of(way):
        return me + 1 if way == 0 else me - 1

    def behind(way):
        return me if way == 0 else mirror

    for way in (1, 0):
        @pl.when(behind(1 - way) > 0)
        def _():
            pl.semaphore_signal(barrier, inc=1, device_id={"space": next_of(way)}, device_id_type=MESH)

    def eig_load(t, d):
        block = pl.ds(pl.multiple_of(d * cols, cols), cols)
        return pltpu.make_async_copy(eig_hbm.at[t, :, :, block], eig_v.at[t, d, :, me], load_sem.at[t, d])

    def sol_copy(t, d):
        owner = pl.ds(d * owned, owned)
        return pltpu.make_async_copy(sol_hbm.at[t, owner], sol_v.at[t, owner], sol_sem.at[t, d])

    def eig_copy(way, t, d, c, s):
        return pltpu.make_async_remote_copy(
            eig_v.at[t, d, c, s], eig_v.at[t, d, c, s], eig_send.at[t, d, c, s], eig_recv.at[t, d, c, s],
            device_id={"space": next_of(way)}, device_id_type=MESH)

    def first_copy(way, t, d, c, s):
        block = pl.ds(pl.multiple_of(d * cols, cols), cols)
        return pltpu.make_async_remote_copy(
            eig_hbm.at[t, c, :, block], eig_v.at[t, d, c, s], eig_send.at[t, d, c, s], eig_recv.at[t, d, c, s],
            device_id={"space": next_of(way)}, device_id_type=MESH)

    def each(total, body):
        def step(i, _):
            body(i)
            return 0
        lax.fori_loop(0, total, step, 0)

    @pl.when(me == 0)
    def _():
        eig_load(0, n - 1).start()

    pl.semaphore_wait(barrier, jnp.where((me > 0) & (mirror > 0), 2, 1))
    @pl.when(me == 0)
    def _():
        eig_load(0, n - 1).wait()
        for c in range(2):
            eig_copy(0, 0, n - 1, c, me).start()

    for c in range(2):
        for way in range(2):
            @pl.when((behind(1 - way) > 0) & (me > 0))
            def _():
                first_copy(way, 0, n - 1 if way == 0 else 0, c, me).start()

    def load_eigs(i):
        far, t = i // slices, i % slices
        for d in (n - 1 - far, far):
            @pl.when((t > 0) | (d == me) | ((d != 0) & (d != n - 1)))
            def _():
                eig_load(t, d).start()

    each(slices * (n // 2), load_eigs)
    if n % 2:
        each(slices, lambda t: eig_load(t, n // 2).start())
    time_copy = pltpu.make_async_copy(time_hbm, time_ref, time_sem)
    time_copy.start()

    def message(way, i):
        members = behind(way) + 1
        slot = i // members
        t, far, back = slot % slices, slot // slices, i % members
        if way == 0:
            return t, n - 1 - far, me - back, far < mirror
        return t, far, me + back, far < me

    def send_eigs(i):
        for c in range(2):
            for way in range(2):
                t, d, s, valid = message(way, i)

                @pl.when(valid)
                def _():
                    @pl.when(s != me)
                    def _():
                        eig_copy(way, t, d, c, s).wait_recv()

                    if c == 0:
                        @pl.when(s == me)
                        def _():
                            eig_load(t, d).wait()

                    eig_copy(way, t, d, c, s).start()

    each(slices * n, lambda i: sol_copy(i // n, i % n).start())
    messages = slices * ((n * n) // 4)
    each(messages - 1, lambda i: send_eigs(i + 1))

    def wait_eigs(t):
        eig_load(t, me).wait()

        def body(i):
            s = i // 2

            @pl.when(s != me)
            def _():
                eig_copy(0, t, me, i % 2, s).wait_recv()

        each(2 * n, body)

    wait_eigs(0)
    each(slices * n, lambda i: sol_copy(i // n, i % n).wait())

    def partial_sum(t, q, dst):
        block = sol_v[t, pl.ds(q * piece, piece)].reshape(rows, cols)
        w = eig_v[t, me]
        if count % 16:
            w = w.astype(jnp.float32)
        w = w.reshape(2 * vectors, cols).astype(jnp.bfloat16)
        p = lax.dot_general(block, w, (((1,), (1,)), ((), ())), preferred_element_type=jnp.float32)
        p = p.reshape(piece, 2, half, 2 * vectors)
        dst[:, :half, :] = p[:, 0, :, :vectors] + p[:, 1, :, vectors:]
        dst[:, half:, :] = p[:, 1, :, :vectors] - p[:, 0, :, vectors:]

    def chunk_copy(way, t, q):
        return pltpu.make_async_remote_copy(
            code.at[t, q], code_in.at[way, t, q], code_send.at[t, q], code_recv.at[way, t, q],
            device_id={"space": jnp.where(way == 0, me + 1, me - 1)}, device_id_type=MESH)

    def head_copy(way, t, q):
        return pltpu.make_async_remote_copy(
            head.at[t, q], head_in.at[way, t, q], head_send.at[t, q], head_recv.at[way, t, q],
            device_id={"space": jnp.where(way == 0, me + 1, me - 1)}, device_id_type=MESH)

    def received(way, t, q):
        head_copy(way, t, q).wait_recv()
        chunk_copy(way, t, q).wait_recv()
        value = code_in[way, t, q].astype(jnp.int32).astype(jnp.float32) * head_in[way, t, q]
        return value.reshape(piece, spins, vectors)

    def emit(way, i):
        far, t, k = i // blocks, (i // pieces) % slices, i % pieces
        d = jnp.where(way == 0, n - 1 - far, far)
        q = d * pieces + k
        partial_sum(t, q, part)

        @pl.when(jnp.where(way == 0, me, mirror) > 0)
        def _():
            part[...] += received(way, t, q)

        x = part[...].reshape(rows, vectors)
        top = jnp.maximum(jnp.max(jnp.abs(x), axis=0, keepdims=True), 1e-30)
        head[t, q] = top * (1.0 / LEVELS)
        code[t, q] = jnp.round(x * (LEVELS / top)).astype(jnp.int32).astype(jnp.int16)
        head_copy(way, t, q).start()
        chunk_copy(way, t, q).start()

    lower = me < n // 2
    early = jnp.where(lower, 0, 1)
    late = 1 - early
    lead = blocks * jnp.where(lower, mirror - me, me - mirror)
    many = blocks * jnp.where(lower, mirror, me)
    few = blocks * jnp.where(lower, me, mirror)

    def emit_step(j):
        if slices > 1:
            @pl.when(j == pieces)
            def _():
                for t in range(1, slices):
                    wait_eigs(t)

        @pl.when((j >= lead) & (j - lead < few))
        def _():
            emit(late, j - lead)

        @pl.when(j < many)
        def _():
            emit(early, j)

    each(blocks * (n - 1), emit_step)

    time_copy.wait()

    def set_sign(j):
        t, b = j // owned, j % owned
        now = lax.axis_index("tm") * slices + t
        value = jnp.where(now < time_ref[me * owned + b], -1.0, 1.0)
        sign[t, b] = jnp.full((1, vectors), value, jnp.float32)

    each(slices * owned, set_sign)
    each(blocks, lambda j: partial_sum(j // pieces, me * pieces + j % pieces, own.at[j // pieces, j % pieces]))

    @pl.when(jnp.where(lower, mirror, me) > 0)
    def _():
        def body(j):
            t, i = j // pieces, j % pieces
            own[t, i] += received(late, t, me * pieces + i)
        each(blocks, body)

    def finish(j):
        t, i = j // pieces, j % pieces
        mine = pl.ds(i * piece, piece)
        inner = jnp.where(lower, me, mirror) > 0

        @pl.when(inner)
        def _():
            total = own[t, i] + received(early, t, me * pieces + i)
            out_ref[t, mine] = (total * sign[t, mine]).astype(jnp.bfloat16)

        @pl.when(jnp.logical_not(inner))
        def _():
            out_ref[t, mine] = (own[t, i] * sign[t, mine]).astype(jnp.bfloat16)

    def drain_eigs(i):
        for c in range(2):
            for way in range(2):
                t, d, s, valid = message(way, i)

                @pl.when(valid)
                def _():
                    eig_copy(way, t, d, c, s).wait_send()


    def drain(j):
        t, q = j // (n * pieces), j % (n * pieces)
        d = q // pieces

        @pl.when(d != me)
        def _():
            way = jnp.where(d > me, 0, 1)
            head_copy(way, t, q).wait_send()
            chunk_copy(way, t, q).wait_send()

    outer = (me == 0) | (mirror == 0)

    @pl.when(outer)
    def _():
        each(blocks, finish)

    each(messages, drain_eigs)
    each(slices * n * pieces, drain)

    @pl.when(jnp.logical_not(outer))
    def _():
        each(blocks, finish)


def shards(n, solutions, eigvecs, source_time):
    slices, sources, spins, cols = solutions.shape
    count = eigvecs.shape[2]
    vectors = n * count
    owned = sources // n
    pieces = PIECES if owned % PIECES == 0 else 1
    piece = owned // pieces
    blocks = n * pieces
    dma = pltpu.SemaphoreType.DMA
    result = jax.ShapeDtypeStruct((slices, owned, spins, vectors), jnp.bfloat16)
    return pl.pallas_call(
        functools.partial(kernel, n, pieces),
        out_shape=result,
        in_specs=[
            pl.BlockSpec(memory_space=pltpu.HBM),
            pl.BlockSpec(memory_space=pltpu.HBM),
            pl.BlockSpec(memory_space=pltpu.HBM),
        ],
        out_specs=pl.BlockSpec(memory_space=pltpu.VMEM),
        scratch_shapes=[
            pltpu.SMEM(source_time.shape, jnp.int32),
            pltpu.VMEM((slices, n, 2, n, count, cols), jnp.bfloat16),
            pltpu.VMEM((slices, sources, spins, cols), jnp.bfloat16),
            pltpu.VMEM((slices, owned, 1, vectors), jnp.float32),
            pltpu.VMEM((piece, spins, vectors), jnp.float32),
            pltpu.VMEM((slices, pieces, piece, spins, vectors), jnp.float32),
            pltpu.VMEM((slices, blocks, piece * spins, vectors), jnp.int16),
            pltpu.VMEM((2, slices, blocks, piece * spins, vectors), jnp.int16),
            pltpu.VMEM((slices, blocks, 1, vectors), jnp.float32),
            pltpu.VMEM((2, slices, blocks, 1, vectors), jnp.float32),
            dma,
            dma((slices, n)),
            dma((slices, n)),
            dma((slices, n, 2, n)),
            dma((slices, n, 2, n)),
            dma((slices, blocks)),
            dma((2, slices, blocks)),
            dma((slices, blocks)),
            dma((2, slices, blocks)),
        ],
        compiler_params=pltpu.CompilerParams(
            collective_id=0, has_side_effects=True, vmem_limit_bytes=VMEM_BYTES),
    )(*(pltpu.with_memory_space_constraint(x, pltpu.HBM) for x in (source_time, solutions, eigvecs)))


def solution(mesh):
    return jax.shard_map(
        functools.partial(shards, mesh.shape["space"]),
        mesh=mesh,
        in_specs=(
            P(("cfg", "tm"), None, None, "space"),
            P(("cfg", "tm"), None, "space", None),
            P("cfg"),
        ),
        out_specs=P(("cfg", "tm"), "space", None, None),
        check_vma=False,
    )
```

```python
import functools

import jax
import jax.numpy as jnp
from jax import lax
from jax.experimental import pallas as pl
from jax.experimental.pallas import tpu as pltpu
from jax.sharding import PartitionSpec as P

MESH = pl.DeviceIdType.MESH
LEVELS = 32767.0
PIECES = 1
SHARE = 2
HELD = 2
VMEM_BYTES = 48 << 20


def kernel(n, pieces, paired, time_hbm, sol_hbm, eig_hbm, out_ref, time_ref, eig_v, sol_v, sign, part, own, code, code_in,
           head, head_in, relay, time_sem, load_sem, sol_sem, eig_send, eig_recv, code_send, code_recv, head_send, head_recv,
           relay_send, relay_recv, relay_hop, relay_land, relay_ready):
    me = lax.axis_index("space")
    slices, sources, spins, cols = sol_v.shape
    count = eig_v.shape[4]
    vectors = n * count
    owned = sources // n
    piece = owned // pieces
    rows = piece * spins
    half = spins // 2
    blocks = slices * pieces
    mirror = n - 1 - me
    outer = (me == 0) | (mirror == 0)
    tm = lax.axis_index("tm")
    hands = (me == 0) & (tm % 2 == 0)
    helps = (me == 0) & (tm % 2 == 1)
    inward = 1
    kept = rows - relay.shape[0]

    barrier = pltpu.get_barrier_semaphore()

    def next_of(way):
        return me + 1 if way == 0 else me - 1

    def behind(way):
        return me if way == 0 else mirror

    for way in (1, 0):
        @pl.when(behind(1 - way) > 0)
        def _():
            pl.semaphore_signal(barrier, inc=1, device_id={"space": next_of(way)}, device_id_type=MESH)

    if paired:
        @pl.when(hands)
        def _():
            pl.semaphore_signal(barrier, inc=1, device_id={"tm": tm + 1}, device_id_type=MESH)

    def eig_load(t, d):
        block = pl.ds(pl.multiple_of(d * cols, cols), cols)
        return pltpu.make_async_copy(eig_hbm.at[t, :, :, block], eig_v.at[t, d, :, me], load_sem.at[t, d])

    def sol_copy(t, d):
        owner = pl.ds(d * owned, owned)
        return pltpu.make_async_copy(sol_hbm.at[t, owner], sol_v.at[t, owner], sol_sem.at[t, d])

    def eig_copy(way, t, d, c, s):
        return pltpu.make_async_remote_copy(
            eig_v.at[t, d, c, s], eig_v.at[t, d, c, s], eig_send.at[t, d, c, s], eig_recv.at[t, d, c, s],
            device_id={"space": next_of(way)}, device_id_type=MESH)

    def first_copy(way, t, d, c, s):
        block = pl.ds(pl.multiple_of(d * cols, cols), cols)
        return pltpu.make_async_remote_copy(
            eig_hbm.at[t, c, :, block], eig_v.at[t, d, c, s], eig_send.at[t, d, c, s], eig_recv.at[t, d, c, s],
            device_id={"space": next_of(way)}, device_id_type=MESH)

    def each(total, body):
        def step(i, _):
            body(i)
            return 0
        lax.fori_loop(0, total, step, 0)

    @pl.when(me == 0)
    def _():
        eig_load(0, n - 1).start()

    if paired:
        pl.semaphore_wait(barrier, jnp.where(outer & jnp.logical_not(helps), 1, 2))

        @pl.when(helps)
        def _():
            pl.semaphore_signal(relay_ready, inc=1, device_id={"tm": tm - 1}, device_id_type=MESH)
    else:
        pl.semaphore_wait(barrier, jnp.where(outer, 1, 2))

    @pl.when(me == 0)
    def _():
        eig_load(0, n - 1).wait()
        for c in range(2):
            eig_copy(0, 0, n - 1, c, me).start()

    for c in range(2):
        for way in range(2):
            @pl.when((behind(1 - way) > 0) & (me > 0))
            def _():
                first_copy(way, 0, n - 1 if way == 0 else 0, c, me).start()

    def load_eigs(i):
        far, t = i // slices, i % slices
        for d in (n - 1 - far, far):
            @pl.when((t > 0) | (d == me) | ((d != 0) & (d != n - 1)))
            def _():
                eig_load(t, d).start()

    each(slices * (n // 2), load_eigs)
    if n % 2:
        each(slices, lambda t: eig_load(t, n // 2).start())
    time_copy = pltpu.make_async_copy(time_hbm, time_ref, time_sem)
    time_copy.start()

    def message(way, i):
        members = behind(way) + 1
        slot = i // members
        t, far, back = slot % slices, slot // slices, i % members
        if way == 0:
            return t, n - 1 - far, me - back, far < mirror
        return t, far, me + back, far < me

    def send_eigs(i):
        for c in range(2):
            for way in range(2):
                t, d, s, valid = message(way, i)

                @pl.when(valid)
                def _():
                    @pl.when(s != me)
                    def _():
                        eig_copy(way, t, d, c, s).wait_recv()

                    if c == 0:
                        @pl.when(s == me)
                        def _():
                            eig_load(t, d).wait()

                    eig_copy(way, t, d, c, s).start()

    each(slices * n, lambda i: sol_copy(i // n, i % n).start())
    messages = slices * ((n * n) // 4)
    each(messages - 1, lambda i: send_eigs(i + 1))

    def wait_eigs(t):
        eig_load(t, me).wait()

        def body(i):
            s = i // 2

            @pl.when(s != me)
            def _():
                eig_copy(0, t, me, i % 2, s).wait_recv()

        each(2 * n, body)

    wait_eigs(0)
    each(slices * n, lambda i: sol_copy(i // n, i % n).wait())

    def partial_sum(t, q, dst):
        block = sol_v[t, pl.ds(q * piece, piece)].reshape(rows, cols)
        w = eig_v[t, me]
        if count % 16:
            w = w.astype(jnp.float32)
        w = w.reshape(2 * vectors, cols).astype(jnp.bfloat16)
        p = lax.dot_general(block, w, (((1,), (1,)), ((), ())), preferred_element_type=jnp.float32)
        p = p.reshape(piece, 2, half, 2 * vectors)
        dst[:, :half, :] = p[:, 0, :, :vectors] + p[:, 1, :, vectors:]
        dst[:, half:, :] = p[:, 1, :, :vectors] - p[:, 0, :, vectors:]

    def chunk_copy(way, t, q):
        return pltpu.make_async_remote_copy(
            code.at[t, q], code_in.at[way, t, q], code_send.at[t, q], code_recv.at[way, t, q],
            device_id={"space": jnp.where(way == 0, me + 1, me - 1)}, device_id_type=MESH)

    def head_copy(way, t, q):
        return pltpu.make_async_remote_copy(
            head.at[t, q], head_in.at[way, t, q], head_send.at[t, q], head_recv.at[way, t, q],
            device_id={"space": jnp.where(way == 0, me + 1, me - 1)}, device_id_type=MESH)

    def kept_copy(way, t, q):
        part = pl.ds(0, kept)
        return pltpu.make_async_remote_copy(
            code.at[t, q, part], code_in.at[way, t, q, part], code_send.at[t, q], code_recv.at[way, t, q],
            device_id={"space": jnp.where(way == 0, me + 1, me - 1)}, device_id_type=MESH)

    def relay_push(t, q):
        return pltpu.make_async_remote_copy(
            code.at[t, q, pl.ds(kept, rows - kept)], relay, relay_send, relay_recv,
            device_id={"tm": tm + 1}, device_id_type=MESH)

    def relay_on(way, t, q):
        return pltpu.make_async_remote_copy(
            relay, code_in.at[way, t, q, pl.ds(kept, rows - kept)], relay_hop, relay_land.at[way],
            device_id={"space": inward, "tm": tm - 1}, device_id_type=MESH)

    def received(way, t, q):
        head_copy(way, t, q).wait_recv()
        if paired:
            parted = (tm % 2 == 0) & (me == 1) & (way == 0) & (t == slices - 1) & (q == me * pieces + pieces - 1)

            @pl.when(parted)
            def _():
                kept_copy(way, t, q).wait_recv()
                relay_on(way, t, q).wait_recv()

            @pl.when(jnp.logical_not(parted))
            def _():
                chunk_copy(way, t, q).wait_recv()
        else:
            chunk_copy(way, t, q).wait_recv()
        value = code_in[way, t, q].astype(jnp.int32).astype(jnp.float32) * head_in[way, t, q]
        return value.reshape(piece, spins, vectors)

    final = blocks * (n - 1) - 1

    def place(way, i):
        far, t, k = i // blocks, (i // pieces) % slices, i % pieces
        return t, jnp.where(way == 0, n - 1 - far, far) * pieces + k

    def emit(way, i):
        t, q = place(way, i)
        partial_sum(t, q, part)

        @pl.when(jnp.where(way == 0, me, mirror) > 0)
        def _():
            part[...] += received(way, t, q)

        x = part[...].reshape(rows, vectors)
        top = jnp.maximum(jnp.max(jnp.abs(x), axis=0, keepdims=True), 1e-30)
        head[t, q] = top * (1.0 / LEVELS)
        code[t, q] = jnp.round(x * (LEVELS / top)).astype(jnp.int32).astype(jnp.int16)
        if paired:
            @pl.when((i == final) & helps)
            def _():
                relay_push(t, q).wait_recv()
                relay_on(way, t, q).start()

            @pl.when(jnp.logical_not(hands & (i >= final - HELD)))
            def _():
                head_copy(way, t, q).start()
                chunk_copy(way, t, q).start()
        else:
            head_copy(way, t, q).start()
            chunk_copy(way, t, q).start()

    lower = me < n // 2
    early = jnp.where(lower, 0, 1)
    late = 1 - early
    lead = blocks * jnp.where(lower, mirror - me, me - mirror)
    many = blocks * jnp.where(lower, mirror, me)
    few = blocks * jnp.where(lower, me, mirror)

    def emit_step(j):
        if slices > 1:
            @pl.when(j == pieces)
            def _():
                for t in range(1, slices):
                    wait_eigs(t)

        @pl.when((j >= lead) & (j - lead < few))
        def _():
            emit(late, j - lead)

        @pl.when(j < many)
        def _():
            emit(early, j)

    each(blocks * (n - 1), emit_step)
    if paired:
        @pl.when(hands)
        def _():
            pl.semaphore_wait(relay_ready, 1)
            relay_push(*place(early, final)).start()

            def start_held(j):
                at = place(early, final - HELD + j)
                head_copy(early, *at).start()
                chunk_copy(early, *at).start()

            each(HELD, start_held)
            at = place(early, final)
            head_copy(early, *at).start()
            kept_copy(early, *at).start()

    time_copy.wait()

    def set_sign(j):
        t, b = j // owned, j % owned
        now = lax.axis_index("tm") * slices + t
        value = jnp.where(now < time_ref[me * owned + b], -1.0, 1.0)
        sign[t, b] = jnp.full((1, vectors), value, jnp.float32)

    each(slices * owned, set_sign)
    each(blocks, lambda j: partial_sum(j // pieces, me * pieces + j % pieces, own.at[j // pieces, j % pieces]))

    @pl.when(jnp.where(lower, mirror, me) > 0)
    def _():
        def body(j):
            t, i = j // pieces, j % pieces
            own[t, i] += received(late, t, me * pieces + i)
        each(blocks, body)

    def finish(j):
        t, i = j // pieces, j % pieces
        mine = pl.ds(i * piece, piece)
        inner = jnp.where(lower, me, mirror) > 0

        @pl.when(inner)
        def _():
            total = own[t, i] + received(early, t, me * pieces + i)
            out_ref[t, mine] = (total * sign[t, mine]).astype(jnp.bfloat16)

        @pl.when(jnp.logical_not(inner))
        def _():
            out_ref[t, mine] = (own[t, i] * sign[t, mine]).astype(jnp.bfloat16)

    def drain_eigs(i):
        for c in range(2):
            for way in range(2):
                t, d, s, valid = message(way, i)

                @pl.when(valid)
                def _():
                    eig_copy(way, t, d, c, s).wait_send()


    def drain(j):
        t, q = j // (n * pieces), j % (n * pieces)
        d = q // pieces

        @pl.when(d != me)
        def _():
            way = jnp.where(d > me, 0, 1)
            head_copy(way, t, q).wait_send()
            if paired:
                last = (me == 0) & (t == slices - 1) & (q == inward * pieces + pieces - 1)

                @pl.when(last & helps)
                def _():
                    relay_on(way, t, q).wait_send()

                @pl.when(last & hands)
                def _():
                    relay_push(t, q).wait_send()
                    kept_copy(way, t, q).wait_send()

                @pl.when(jnp.logical_not(last & hands))
                def _():
                    chunk_copy(way, t, q).wait_send()
            else:
                chunk_copy(way, t, q).wait_send()

    @pl.when(outer)
    def _():
        each(blocks, finish)

    each(messages, drain_eigs)
    each(slices * n * pieces, drain)

    @pl.when(jnp.logical_not(outer))
    def _():
        each(blocks, finish)


def shards(n, cores, solutions, eigvecs, source_time):
    slices, sources, spins, cols = solutions.shape
    count = eigvecs.shape[2]
    vectors = n * count
    owned = sources // n
    pieces = PIECES if owned % PIECES == 0 else 1
    piece = owned // pieces
    blocks = n * pieces
    dma = pltpu.SemaphoreType.DMA
    result = jax.ShapeDtypeStruct((slices, owned, spins, vectors), jnp.bfloat16)
    return pl.pallas_call(
        functools.partial(kernel, n, pieces, cores % 2 == 0),
        out_shape=result,
        in_specs=[
            pl.BlockSpec(memory_space=pltpu.HBM),
            pl.BlockSpec(memory_space=pltpu.HBM),
            pl.BlockSpec(memory_space=pltpu.HBM),
        ],
        out_specs=pl.BlockSpec(memory_space=pltpu.VMEM),
        scratch_shapes=[
            pltpu.SMEM(source_time.shape, jnp.int32),
            pltpu.VMEM((slices, n, 2, n, count, cols), jnp.bfloat16),
            pltpu.VMEM((slices, sources, spins, cols), jnp.bfloat16),
            pltpu.VMEM((slices, owned, 1, vectors), jnp.float32),
            pltpu.VMEM((piece, spins, vectors), jnp.float32),
            pltpu.VMEM((slices, pieces, piece, spins, vectors), jnp.float32),
            pltpu.VMEM((slices, blocks, piece * spins, vectors), jnp.int16),
            pltpu.VMEM((2, slices, blocks, piece * spins, vectors), jnp.int16),
            pltpu.VMEM((slices, blocks, 1, vectors), jnp.float32),
            pltpu.VMEM((2, slices, blocks, 1, vectors), jnp.float32),
            pltpu.VMEM((piece * spins // SHARE, vectors), jnp.int16),
            dma,
            dma((slices, n)),
            dma((slices, n)),
            dma((slices, n, 2, n)),
            dma((slices, n, 2, n)),
            dma((slices, blocks)),
            dma((2, slices, blocks)),
            dma((slices, blocks)),
            dma((2, slices, blocks)),
            dma,
            dma,
            dma,
            dma((2,)),
            pltpu.SemaphoreType.REGULAR,
        ],
        compiler_params=pltpu.CompilerParams(
            collective_id=0, has_side_effects=True, vmem_limit_bytes=VMEM_BYTES),
    )(*(pltpu.with_memory_space_constraint(x, pltpu.HBM) for x in (source_time, solutions, eigvecs)))


def solution(mesh):
    return jax.shard_map(
        functools.partial(shards, mesh.shape["space"], mesh.shape["tm"]),
        mesh=mesh,
        in_specs=(
            P(("cfg", "tm"), None, None, "space"),
            P(("cfg", "tm"), None, "space", None),
            P("cfg"),
        ),
        out_specs=P(("cfg", "tm"), "space", None, None),
        check_vma=False,
    )
```

```python
import functools

import jax
import jax.numpy as jnp
from jax import lax
from jax.experimental import pallas as pl
from jax.experimental.pallas import tpu as pltpu
from jax.sharding import PartitionSpec as P

MESH = pl.DeviceIdType.MESH
LEVELS = 32767.0
PIECES = 1
SHARE = 2
HELD = 2
VMEM_BYTES = 48 << 20


def kernel(n, pieces, paired, time_hbm, sol_hbm, eig_hbm, out_ref, time_ref, eig_v, sol_v, sign, part, own, code, code_in,
           head, head_in, relay, time_sem, load_sem, sol_sem, eig_send, eig_recv, code_send, code_recv, head_send, head_recv,
           relay_send, relay_recv, relay_hop, relay_land):
    me = lax.axis_index("space")
    slices, sources, spins, cols = sol_v.shape
    count = eig_v.shape[4]
    vectors = n * count
    owned = sources // n
    piece = owned // pieces
    rows = piece * spins
    half = spins // 2
    blocks = slices * pieces
    mirror = n - 1 - me
    outer = (me == 0) | (mirror == 0)
    tm = lax.axis_index("tm")
    hands = outer & (tm % 2 == 0)
    helps = outer & (tm % 2 == 1)
    inward = jnp.where(me == 0, 1, n - 2)
    kept = rows - relay.shape[0]

    barrier = pltpu.get_barrier_semaphore()

    def next_of(way):
        return me + 1 if way == 0 else me - 1

    def behind(way):
        return me if way == 0 else mirror

    for way in (1, 0):
        @pl.when(behind(1 - way) > 0)
        def _():
            pl.semaphore_signal(barrier, inc=1, device_id={"space": next_of(way)}, device_id_type=MESH)

    if paired:
        @pl.when(helps)
        def _():
            pl.semaphore_signal(barrier, inc=1, device_id={"tm": tm - 1}, device_id_type=MESH)

    def eig_load(t, d):
        block = pl.ds(pl.multiple_of(d * cols, cols), cols)
        return pltpu.make_async_copy(eig_hbm.at[t, :, :, block], eig_v.at[t, d, :, me], load_sem.at[t, d])

    def sol_copy(t, d):
        owner = pl.ds(d * owned, owned)
        return pltpu.make_async_copy(sol_hbm.at[t, owner], sol_v.at[t, owner], sol_sem.at[t, d])

    def eig_copy(way, t, d, c, s):
        return pltpu.make_async_remote_copy(
            eig_v.at[t, d, c, s], eig_v.at[t, d, c, s], eig_send.at[t, d, c, s], eig_recv.at[t, d, c, s],
            device_id={"space": next_of(way)}, device_id_type=MESH)

    def first_copy(way, t, d, c, s):
        block = pl.ds(pl.multiple_of(d * cols, cols), cols)
        return pltpu.make_async_remote_copy(
            eig_hbm.at[t, c, :, block], eig_v.at[t, d, c, s], eig_send.at[t, d, c, s], eig_recv.at[t, d, c, s],
            device_id={"space": next_of(way)}, device_id_type=MESH)

    def each(total, body):
        def step(i, _):
            body(i)
            return 0
        lax.fori_loop(0, total, step, 0)

    @pl.when(me == 0)
    def _():
        eig_load(0, n - 1).start()

    pl.semaphore_wait(barrier, jnp.where(outer & jnp.logical_not(hands & paired), 1, 2))

    @pl.when(me == 0)
    def _():
        eig_load(0, n - 1).wait()
        for c in range(2):
            eig_copy(0, 0, n - 1, c, me).start()

    for c in range(2):
        for way in range(2):
            @pl.when((behind(1 - way) > 0) & (me > 0))
            def _():
                first_copy(way, 0, n - 1 if way == 0 else 0, c, me).start()

    def load_eigs(i):
        far, t = i // slices, i % slices
        for d in (n - 1 - far, far):
            @pl.when((t > 0) | (d == me) | ((d != 0) & (d != n - 1)))
            def _():
                eig_load(t, d).start()

    each(slices * (n // 2), load_eigs)
    if n % 2:
        each(slices, lambda t: eig_load(t, n // 2).start())
    time_copy = pltpu.make_async_copy(time_hbm, time_ref, time_sem)
    time_copy.start()

    def message(way, i):
        members = behind(way) + 1
        slot = i // members
        t, far, back = slot % slices, slot // slices, i % members
        if way == 0:
            return t, n - 1 - far, me - back, far < mirror
        return t, far, me + back, far < me

    def send_eigs(i):
        for c in range(2):
            for way in range(2):
                t, d, s, valid = message(way, i)

                @pl.when(valid)
                def _():
                    @pl.when(s != me)
                    def _():
                        eig_copy(way, t, d, c, s).wait_recv()

                    if c == 0:
                        @pl.when(s == me)
                        def _():
                            eig_load(t, d).wait()

                    eig_copy(way, t, d, c, s).start()

    each(slices * n, lambda i: sol_copy(i // n, i % n).start())
    messages = slices * ((n * n) // 4)
    each(messages - 1, lambda i: send_eigs(i + 1))

    def wait_eigs(t):
        eig_load(t, me).wait()

        def body(i):
            s = i // 2

            @pl.when(s != me)
            def _():
                eig_copy(0, t, me, i % 2, s).wait_recv()

        each(2 * n, body)

    wait_eigs(0)
    each(slices * n, lambda i: sol_copy(i // n, i % n).wait())

    def partial_sum(t, q, dst):
        block = sol_v[t, pl.ds(q * piece, piece)].reshape(rows, cols)
        w = eig_v[t, me]
        if count % 16:
            w = w.astype(jnp.float32)
        w = w.reshape(2 * vectors, cols).astype(jnp.bfloat16)
        p = lax.dot_general(block, w, (((1,), (1,)), ((), ())), preferred_element_type=jnp.float32)
        p = p.reshape(piece, 2, half, 2 * vectors)
        dst[:, :half, :] = p[:, 0, :, :vectors] + p[:, 1, :, vectors:]
        dst[:, half:, :] = p[:, 1, :, :vectors] - p[:, 0, :, vectors:]

    def chunk_copy(way, t, q):
        return pltpu.make_async_remote_copy(
            code.at[t, q], code_in.at[way, t, q], code_send.at[t, q], code_recv.at[way, t, q],
            device_id={"space": jnp.where(way == 0, me + 1, me - 1)}, device_id_type=MESH)

    def head_copy(way, t, q):
        return pltpu.make_async_remote_copy(
            head.at[t, q], head_in.at[way, t, q], head_send.at[t, q], head_recv.at[way, t, q],
            device_id={"space": jnp.where(way == 0, me + 1, me - 1)}, device_id_type=MESH)

    def kept_copy(way, t, q):
        part = pl.ds(0, kept)
        return pltpu.make_async_remote_copy(
            code.at[t, q, part], code_in.at[way, t, q, part], code_send.at[t, q], code_recv.at[way, t, q],
            device_id={"space": jnp.where(way == 0, me + 1, me - 1)}, device_id_type=MESH)

    def relay_push(t, q):
        return pltpu.make_async_remote_copy(
            code.at[t, q, pl.ds(kept, rows - kept)], relay, relay_send, relay_recv,
            device_id={"tm": tm + 1}, device_id_type=MESH)

    def relay_on(way, t, q):
        return pltpu.make_async_remote_copy(
            relay, code_in.at[way, t, q, pl.ds(kept, rows - kept)], relay_hop, relay_land.at[way],
            device_id={"space": inward, "tm": tm - 1}, device_id_type=MESH)

    def received(way, t, q):
        head_copy(way, t, q).wait_recv()
        if paired:
            from_end = jnp.where(way == 0, me == 1, mirror == 1)
            parted = (tm % 2 == 0) & from_end & (t == slices - 1) & (q == me * pieces + pieces - 1)

            @pl.when(parted)
            def _():
                kept_copy(way, t, q).wait_recv()
                relay_on(way, t, q).wait_recv()

            @pl.when(jnp.logical_not(parted))
            def _():
                chunk_copy(way, t, q).wait_recv()
        else:
            chunk_copy(way, t, q).wait_recv()
        value = code_in[way, t, q].astype(jnp.int32).astype(jnp.float32) * head_in[way, t, q]
        return value.reshape(piece, spins, vectors)

    final = blocks * (n - 1) - 1

    def place(way, i):
        far, t, k = i // blocks, (i // pieces) % slices, i % pieces
        return t, jnp.where(way == 0, n - 1 - far, far) * pieces + k

    def emit(way, i):
        t, q = place(way, i)
        partial_sum(t, q, part)

        @pl.when(jnp.where(way == 0, me, mirror) > 0)
        def _():
            part[...] += received(way, t, q)

        x = part[...].reshape(rows, vectors)
        top = jnp.maximum(jnp.max(jnp.abs(x), axis=0, keepdims=True), 1e-30)
        head[t, q] = top * (1.0 / LEVELS)
        code[t, q] = jnp.round(x * (LEVELS / top)).astype(jnp.int32).astype(jnp.int16)
        if paired:
            @pl.when((i == final) & helps)
            def _():
                relay_push(t, q).wait_recv()
                relay_on(way, t, q).start()

            @pl.when(jnp.logical_not(hands & (i >= final - HELD)))
            def _():
                head_copy(way, t, q).start()
                chunk_copy(way, t, q).start()
        else:
            head_copy(way, t, q).start()
            chunk_copy(way, t, q).start()

    lower = me < n // 2
    early = jnp.where(lower, 0, 1)
    late = 1 - early
    lead = blocks * jnp.where(lower, mirror - me, me - mirror)
    many = blocks * jnp.where(lower, mirror, me)
    few = blocks * jnp.where(lower, me, mirror)

    def emit_step(j):
        if slices > 1:
            @pl.when(j == pieces)
            def _():
                for t in range(1, slices):
                    wait_eigs(t)

        @pl.when((j >= lead) & (j - lead < few))
        def _():
            emit(late, j - lead)

        @pl.when(j < many)
        def _():
            emit(early, j)

    each(blocks * (n - 1), emit_step)
    if paired:
        @pl.when(hands)
        def _():
            relay_push(*place(early, final)).start()

            def start_held(j):
                at = place(early, final - HELD + j)
                head_copy(early, *at).start()
                chunk_copy(early, *at).start()

            each(HELD, start_held)
            at = place(early, final)
            head_copy(early, *at).start()
            kept_copy(early, *at).start()

    time_copy.wait()

    def set_sign(j):
        t, b = j // owned, j % owned
        now = lax.axis_index("tm") * slices + t
        value = jnp.where(now < time_ref[me * owned + b], -1.0, 1.0)
        sign[t, b] = jnp.full((1, vectors), value, jnp.float32)

    each(slices * owned, set_sign)
    each(blocks, lambda j: partial_sum(j // pieces, me * pieces + j % pieces, own.at[j // pieces, j % pieces]))

    @pl.when(jnp.where(lower, mirror, me) > 0)
    def _():
        def body(j):
            t, i = j // pieces, j % pieces
            own[t, i] += received(late, t, me * pieces + i)
        each(blocks, body)

    def finish(j):
        t, i = j // pieces, j % pieces
        mine = pl.ds(i * piece, piece)
        inner = jnp.where(lower, me, mirror) > 0

        @pl.when(inner)
        def _():
            total = own[t, i] + received(early, t, me * pieces + i)
            out_ref[t, mine] = (total * sign[t, mine]).astype(jnp.bfloat16)

        @pl.when(jnp.logical_not(inner))
        def _():
            out_ref[t, mine] = (own[t, i] * sign[t, mine]).astype(jnp.bfloat16)

    def drain_eigs(i):
        for c in range(2):
            for way in range(2):
                t, d, s, valid = message(way, i)

                @pl.when(valid)
                def _():
                    eig_copy(way, t, d, c, s).wait_send()


    def drain(j):
        t, q = j // (n * pieces), j % (n * pieces)
        d = q // pieces

        @pl.when(d != me)
        def _():
            way = jnp.where(d > me, 0, 1)
            head_copy(way, t, q).wait_send()
            if paired:
                last = outer & (t == slices - 1) & (q == inward * pieces + pieces - 1)

                @pl.when(last & helps)
                def _():
                    relay_on(way, t, q).wait_send()

                @pl.when(last & hands)
                def _():
                    relay_push(t, q).wait_send()
                    kept_copy(way, t, q).wait_send()

                @pl.when(jnp.logical_not(last & hands))
                def _():
                    chunk_copy(way, t, q).wait_send()
            else:
                chunk_copy(way, t, q).wait_send()

    @pl.when(outer)
    def _():
        each(blocks, finish)

    each(messages, drain_eigs)
    each(slices * n * pieces, drain)

    @pl.when(jnp.logical_not(outer))
    def _():
        each(blocks, finish)


def shards(n, cores, solutions, eigvecs, source_time):
    slices, sources, spins, cols = solutions.shape
    count = eigvecs.shape[2]
    vectors = n * count
    owned = sources // n
    pieces = PIECES if owned % PIECES == 0 else 1
    piece = owned // pieces
    blocks = n * pieces
    dma = pltpu.SemaphoreType.DMA
    result = jax.ShapeDtypeStruct((slices, owned, spins, vectors), jnp.bfloat16)
    return pl.pallas_call(
        functools.partial(kernel, n, pieces, cores % 2 == 0),
        out_shape=result,
        in_specs=[
            pl.BlockSpec(memory_space=pltpu.HBM),
            pl.BlockSpec(memory_space=pltpu.HBM),
            pl.BlockSpec(memory_space=pltpu.HBM),
        ],
        out_specs=pl.BlockSpec(memory_space=pltpu.VMEM),
        scratch_shapes=[
            pltpu.SMEM(source_time.shape, jnp.int32),
            pltpu.VMEM((slices, n, 2, n, count, cols), jnp.bfloat16),
            pltpu.VMEM((slices, sources, spins, cols), jnp.bfloat16),
            pltpu.VMEM((slices, owned, 1, vectors), jnp.float32),
            pltpu.VMEM((piece, spins, vectors), jnp.float32),
            pltpu.VMEM((slices, pieces, piece, spins, vectors), jnp.float32),
            pltpu.VMEM((slices, blocks, piece * spins, vectors), jnp.int16),
            pltpu.VMEM((2, slices, blocks, piece * spins, vectors), jnp.int16),
            pltpu.VMEM((slices, blocks, 1, vectors), jnp.float32),
            pltpu.VMEM((2, slices, blocks, 1, vectors), jnp.float32),
            pltpu.VMEM((piece * spins // SHARE, vectors), jnp.int16),
            dma,
            dma((slices, n)),
            dma((slices, n)),
            dma((slices, n, 2, n)),
            dma((slices, n, 2, n)),
            dma((slices, blocks)),
            dma((2, slices, blocks)),
            dma((slices, blocks)),
            dma((2, slices, blocks)),
            dma,
            dma,
            dma,
            dma((2,)),
        ],
        compiler_params=pltpu.CompilerParams(
            collective_id=0, has_side_effects=True, vmem_limit_bytes=VMEM_BYTES),
    )(*(pltpu.with_memory_space_constraint(x, pltpu.HBM) for x in (source_time, solutions, eigvecs)))


def solution(mesh):
    return jax.shard_map(
        functools.partial(shards, mesh.shape["space"], mesh.shape["tm"]),
        mesh=mesh,
        in_specs=(
            P(("cfg", "tm"), None, None, "space"),
            P(("cfg", "tm"), None, "space", None),
            P("cfg"),
        ),
        out_specs=P(("cfg", "tm"), "space", None, None),
        check_vma=False,
    )
```

```python
import functools

import jax
import jax.numpy as jnp
from jax import lax
from jax.experimental import pallas as pl
from jax.experimental.pallas import tpu as pltpu
from jax.sharding import PartitionSpec as P

MESH = pl.DeviceIdType.MESH
LEVELS = 32767.0
PIECES = 1
SHARE = 2
HELD = 1
VMEM_BYTES = 48 << 20


def kernel(n, pieces, paired, time_hbm, sol_hbm, eig_hbm, out_ref, time_ref, eig_v, sol_v, sign, part, own, code, code_in,
           head, head_in, relay, time_sem, load_sem, sol_sem, eig_send, eig_recv, code_send, code_recv, head_send, head_recv,
           relay_send, relay_recv, relay_hop, relay_land):
    me = lax.axis_index("space")
    slices, sources, spins, cols = sol_v.shape
    count = eig_v.shape[4]
    vectors = n * count
    owned = sources // n
    piece = owned // pieces
    rows = piece * spins
    half = spins // 2
    blocks = slices * pieces
    mirror = n - 1 - me
    outer = (me == 0) | (mirror == 0)
    tm = lax.axis_index("tm")
    hands = outer & (tm % 2 == 0)
    helps = outer & (tm % 2 == 1)
    inward = jnp.where(me == 0, 1, n - 2)
    kept = rows - relay.shape[0]

    barrier = pltpu.get_barrier_semaphore()

    def next_of(way):
        return me + 1 if way == 0 else me - 1

    def behind(way):
        return me if way == 0 else mirror

    for way in (1, 0):
        @pl.when(behind(1 - way) > 0)
        def _():
            pl.semaphore_signal(barrier, inc=1, device_id={"space": next_of(way)}, device_id_type=MESH)

    if paired:
        @pl.when(helps)
        def _():
            pl.semaphore_signal(barrier, inc=1, device_id={"tm": tm - 1}, device_id_type=MESH)

    def eig_load(t, d):
        block = pl.ds(pl.multiple_of(d * cols, cols), cols)
        return pltpu.make_async_copy(eig_hbm.at[t, :, :, block], eig_v.at[t, d, :, me], load_sem.at[t, d])

    def sol_copy(t, d):
        owner = pl.ds(d * owned, owned)
        return pltpu.make_async_copy(sol_hbm.at[t, owner], sol_v.at[t, owner], sol_sem.at[t, d])

    def eig_copy(way, t, d, c, s):
        return pltpu.make_async_remote_copy(
            eig_v.at[t, d, c, s], eig_v.at[t, d, c, s], eig_send.at[t, d, c, s], eig_recv.at[t, d, c, s],
            device_id={"space": next_of(way)}, device_id_type=MESH)

    def first_copy(way, t, d, c, s):
        block = pl.ds(pl.multiple_of(d * cols, cols), cols)
        return pltpu.make_async_remote_copy(
            eig_hbm.at[t, c, :, block], eig_v.at[t, d, c, s], eig_send.at[t, d, c, s], eig_recv.at[t, d, c, s],
            device_id={"space": next_of(way)}, device_id_type=MESH)

    def each(total, body):
        def step(i, _):
            body(i)
            return 0
        lax.fori_loop(0, total, step, 0)

    @pl.when(me == 0)
    def _():
        eig_load(0, n - 1).start()

    pl.semaphore_wait(barrier, jnp.where(outer & jnp.logical_not(hands & paired), 1, 2))

    @pl.when(me == 0)
    def _():
        eig_load(0, n - 1).wait()
        for c in range(2):
            eig_copy(0, 0, n - 1, c, me).start()

    for c in range(2):
        for way in range(2):
            @pl.when((behind(1 - way) > 0) & (me > 0))
            def _():
                first_copy(way, 0, n - 1 if way == 0 else 0, c, me).start()

    def load_eigs(i):
        far, t = i // slices, i % slices
        for d in (n - 1 - far, far):
            @pl.when((t > 0) | (d == me) | ((d != 0) & (d != n - 1)))
            def _():
                eig_load(t, d).start()

    each(slices * (n // 2), load_eigs)
    if n % 2:
        each(slices, lambda t: eig_load(t, n // 2).start())
    time_copy = pltpu.make_async_copy(time_hbm, time_ref, time_sem)
    time_copy.start()

    def message(way, i):
        members = behind(way) + 1
        slot = i // members
        t, far, back = slot % slices, slot // slices, i % members
        if way == 0:
            return t, n - 1 - far, me - back, far < mirror
        return t, far, me + back, far < me

    def send_eigs(i):
        for c in range(2):
            for way in range(2):
                t, d, s, valid = message(way, i)

                @pl.when(valid)
                def _():
                    @pl.when(s != me)
                    def _():
                        eig_copy(way, t, d, c, s).wait_recv()

                    if c == 0:
                        @pl.when(s == me)
                        def _():
                            eig_load(t, d).wait()

                    eig_copy(way, t, d, c, s).start()

    each(slices * n, lambda i: sol_copy(i // n, i % n).start())
    messages = slices * ((n * n) // 4)
    each(messages - 1, lambda i: send_eigs(i + 1))

    def wait_eigs(t):
        eig_load(t, me).wait()

        def body(i):
            s = i // 2

            @pl.when(s != me)
            def _():
                eig_copy(0, t, me, i % 2, s).wait_recv()

        each(2 * n, body)

    wait_eigs(0)
    each(slices * n, lambda i: sol_copy(i // n, i % n).wait())

    def partial_sum(t, q, dst):
        block = sol_v[t, pl.ds(q * piece, piece)].reshape(rows, cols)
        w = eig_v[t, me]
        if count % 16:
            w = w.astype(jnp.float32)
        w = w.reshape(2 * vectors, cols).astype(jnp.bfloat16)
        p = lax.dot_general(block, w, (((1,), (1,)), ((), ())), preferred_element_type=jnp.float32)
        p = p.reshape(piece, 2, half, 2 * vectors)
        dst[:, :half, :] = p[:, 0, :, :vectors] + p[:, 1, :, vectors:]
        dst[:, half:, :] = p[:, 1, :, :vectors] - p[:, 0, :, vectors:]

    def chunk_copy(way, t, q):
        return pltpu.make_async_remote_copy(
            code.at[t, q], code_in.at[way, t, q], code_send.at[t, q], code_recv.at[way, t, q],
            device_id={"space": jnp.where(way == 0, me + 1, me - 1)}, device_id_type=MESH)

    def head_copy(way, t, q):
        return pltpu.make_async_remote_copy(
            head.at[t, q], head_in.at[way, t, q], head_send.at[t, q], head_recv.at[way, t, q],
            device_id={"space": jnp.where(way == 0, me + 1, me - 1)}, device_id_type=MESH)

    def kept_copy(way, t, q):
        part = pl.ds(0, kept)
        return pltpu.make_async_remote_copy(
            code.at[t, q, part], code_in.at[way, t, q, part], code_send.at[t, q], code_recv.at[way, t, q],
            device_id={"space": jnp.where(way == 0, me + 1, me - 1)}, device_id_type=MESH)

    def relay_push(t, q):
        return pltpu.make_async_remote_copy(
            code.at[t, q, pl.ds(kept, rows - kept)], relay, relay_send, relay_recv,
            device_id={"tm": tm + 1}, device_id_type=MESH)

    def relay_on(way, t, q):
        return pltpu.make_async_remote_copy(
            relay, code_in.at[way, t, q, pl.ds(kept, rows - kept)], relay_hop, relay_land.at[way],
            device_id={"space": inward, "tm": tm - 1}, device_id_type=MESH)

    def received(way, t, q):
        head_copy(way, t, q).wait_recv()
        if paired:
            from_end = jnp.where(way == 0, me == 1, mirror == 1)
            parted = (tm % 2 == 0) & from_end & (t == slices - 1) & (q == me * pieces + pieces - 1)

            @pl.when(parted)
            def _():
                kept_copy(way, t, q).wait_recv()
                relay_on(way, t, q).wait_recv()

            @pl.when(jnp.logical_not(parted))
            def _():
                chunk_copy(way, t, q).wait_recv()
        else:
            chunk_copy(way, t, q).wait_recv()
        value = code_in[way, t, q].astype(jnp.int32).astype(jnp.float32) * head_in[way, t, q]
        return value.reshape(piece, spins, vectors)

    final = blocks * (n - 1) - 1
    held = min(HELD, final)

    def place(way, i):
        far, t, k = i // blocks, (i // pieces) % slices, i % pieces
        return t, jnp.where(way == 0, n - 1 - far, far) * pieces + k

    def emit(way, i):
        t, q = place(way, i)
        partial_sum(t, q, part)

        @pl.when(jnp.where(way == 0, me, mirror) > 0)
        def _():
            part[...] += received(way, t, q)

        x = part[...].reshape(rows, vectors)
        top = jnp.maximum(jnp.max(jnp.abs(x), axis=0, keepdims=True), 1e-30)
        head[t, q] = top * (1.0 / LEVELS)
        code[t, q] = jnp.round(x * (LEVELS / top)).astype(jnp.int32).astype(jnp.int16)
        if paired:
            @pl.when((i == final) & helps)
            def _():
                relay_push(t, q).wait_recv()
                relay_on(way, t, q).start()

            @pl.when(jnp.logical_not(hands & (i >= final - held)))
            def _():
                head_copy(way, t, q).start()
                chunk_copy(way, t, q).start()
        else:
            head_copy(way, t, q).start()
            chunk_copy(way, t, q).start()

    lower = me < n // 2
    early = jnp.where(lower, 0, 1)
    late = 1 - early
    lead = blocks * jnp.where(lower, mirror - me, me - mirror)
    many = blocks * jnp.where(lower, mirror, me)
    few = blocks * jnp.where(lower, me, mirror)

    def emit_step(j):
        if slices > 1:
            @pl.when(j == pieces)
            def _():
                for t in range(1, slices):
                    wait_eigs(t)

        @pl.when((j >= lead) & (j - lead < few))
        def _():
            emit(late, j - lead)

        @pl.when(j < many)
        def _():
            emit(early, j)

    each(blocks * (n - 1), emit_step)
    if paired:
        @pl.when(hands)
        def _():
            relay_push(*place(early, final)).start()

            def start_held(j):
                at = place(early, final - held + j)
                head_copy(early, *at).start()
                chunk_copy(early, *at).start()

            each(held, start_held)
            at = place(early, final)
            head_copy(early, *at).start()
            kept_copy(early, *at).start()

    time_copy.wait()

    def set_sign(j):
        t, b = j // owned, j % owned
        now = lax.axis_index("tm") * slices + t
        value = jnp.where(now < time_ref[me * owned + b], -1.0, 1.0)
        sign[t, b] = jnp.full((1, vectors), value, jnp.float32)

    each(slices * owned, set_sign)
    each(blocks, lambda j: partial_sum(j // pieces, me * pieces + j % pieces, own.at[j // pieces, j % pieces]))

    @pl.when(jnp.where(lower, mirror, me) > 0)
    def _():
        def body(j):
            t, i = j // pieces, j % pieces
            own[t, i] += received(late, t, me * pieces + i)
        each(blocks, body)

    def finish(j):
        t, i = j // pieces, j % pieces
        mine = pl.ds(i * piece, piece)
        inner = jnp.where(lower, me, mirror) > 0

        @pl.when(inner)
        def _():
            total = own[t, i] + received(early, t, me * pieces + i)
            out_ref[t, mine] = (total * sign[t, mine]).astype(jnp.bfloat16)

        @pl.when(jnp.logical_not(inner))
        def _():
            out_ref[t, mine] = (own[t, i] * sign[t, mine]).astype(jnp.bfloat16)

    def drain_eigs(i):
        for c in range(2):
            for way in range(2):
                t, d, s, valid = message(way, i)

                @pl.when(valid)
                def _():
                    eig_copy(way, t, d, c, s).wait_send()


    def drain(j):
        t, q = j // (n * pieces), j % (n * pieces)
        d = q // pieces

        @pl.when(d != me)
        def _():
            way = jnp.where(d > me, 0, 1)
            head_copy(way, t, q).wait_send()
            if paired:
                last = outer & (t == slices - 1) & (q == inward * pieces + pieces - 1)

                @pl.when(last & helps)
                def _():
                    relay_on(way, t, q).wait_send()

                @pl.when(last & hands)
                def _():
                    relay_push(t, q).wait_send()
                    kept_copy(way, t, q).wait_send()

                @pl.when(jnp.logical_not(last & hands))
                def _():
                    chunk_copy(way, t, q).wait_send()
            else:
                chunk_copy(way, t, q).wait_send()

    @pl.when(outer)
    def _():
        each(blocks, finish)

    each(messages, drain_eigs)
    each(slices * n * pieces, drain)

    @pl.when(jnp.logical_not(outer))
    def _():
        each(blocks, finish)


def shards(n, cores, solutions, eigvecs, source_time):
    slices, sources, spins, cols = solutions.shape
    count = eigvecs.shape[2]
    vectors = n * count
    owned = sources // n
    pieces = PIECES if owned % PIECES == 0 else 1
    piece = owned // pieces
    blocks = n * pieces
    dma = pltpu.SemaphoreType.DMA
    result = jax.ShapeDtypeStruct((slices, owned, spins, vectors), jnp.bfloat16)
    return pl.pallas_call(
        functools.partial(kernel, n, pieces, cores % 2 == 0),
        out_shape=result,
        in_specs=[
            pl.BlockSpec(memory_space=pltpu.HBM),
            pl.BlockSpec(memory_space=pltpu.HBM),
            pl.BlockSpec(memory_space=pltpu.HBM),
        ],
        out_specs=pl.BlockSpec(memory_space=pltpu.VMEM),
        scratch_shapes=[
            pltpu.SMEM(source_time.shape, jnp.int32),
            pltpu.VMEM((slices, n, 2, n, count, cols), jnp.bfloat16),
            pltpu.VMEM((slices, sources, spins, cols), jnp.bfloat16),
            pltpu.VMEM((slices, owned, 1, vectors), jnp.float32),
            pltpu.VMEM((piece, spins, vectors), jnp.float32),
            pltpu.VMEM((slices, pieces, piece, spins, vectors), jnp.float32),
            pltpu.VMEM((slices, blocks, piece * spins, vectors), jnp.int16),
            pltpu.VMEM((2, slices, blocks, piece * spins, vectors), jnp.int16),
            pltpu.VMEM((slices, blocks, 1, vectors), jnp.float32),
            pltpu.VMEM((2, slices, blocks, 1, vectors), jnp.float32),
            pltpu.VMEM((piece * spins // SHARE, vectors), jnp.int16),
            dma,
            dma((slices, n)),
            dma((slices, n)),
            dma((slices, n, 2, n)),
            dma((slices, n, 2, n)),
            dma((slices, blocks)),
            dma((2, slices, blocks)),
            dma((slices, blocks)),
            dma((2, slices, blocks)),
            dma,
            dma,
            dma,
            dma((2,)),
        ],
        compiler_params=pltpu.CompilerParams(
            collective_id=0, has_side_effects=True, vmem_limit_bytes=VMEM_BYTES),
    )(*(pltpu.with_memory_space_constraint(x, pltpu.HBM) for x in (source_time, solutions, eigvecs)))


def solution(mesh):
    return jax.shard_map(
        functools.partial(shards, mesh.shape["space"], mesh.shape["tm"]),
        mesh=mesh,
        in_specs=(
            P(("cfg", "tm"), None, None, "space"),
            P(("cfg", "tm"), None, "space", None),
            P("cfg"),
        ),
        out_specs=P(("cfg", "tm"), "space", None, None),
        check_vma=False,
    )
```
